512 devices in a mesh: out: 16 (over x_hi, y), in: 32 (over x_lo, z, core).
Axes of the slice: x: 4 (x_hi: 2, x_lo: 2; x = x_hi * 2 + x_lo), y: 8, z: 8, core: 2. Of those that a mesh axis runs over, the one named last changes fastest.
Arguments:
- gradients: bfloat16 [1024, 28672], P('out', 'in'), may hold values from -6 to 6
- activations: bfloat16 [1024, 8192], P('in', 'out'), may hold values from -6 to 6
- out_basis: bfloat16 [28672, 14336], P('in', 'out'), may hold values from -0.03125 to 0.03125
- in_basis: bfloat16 [8192, 8192], P('out', 'in'), may hold values from -0.0625 to 0.0625
- eigen_table: float32 [14336, 8192], P('out', 'in'), may hold values from 0.1 to 2
Outputs:
- updated_table: float32 [14336, 8192], P('out', 'in')
The draws below stay inside these ranges and needn't reach their ends.
All inputs are finite; a program needn't handle non-finite values.
Results may differ from the reference program's by a relative error of at most 0.002.
Values may be sent and summed in bfloat16 or wider, within the bound.
No kernel may reach another device: no remote copies, remote signals or barrier semaphores. Data moves between devices by JAX's collectives and lax.ppermute only.
A program may use at most 64 MiB of HBM per device.

```python
import math
import jax
import jax.numpy as jnp
from jax import lax

OUT_DIM = 28672
IN_DIM = 8192
EIG_OUT = 14336
LEN = 128
SEQS = 8
TOKENS = 1024


def steps_of(key, dims, shards, smallest, high):
    def one(dim, shards_of):
        steps = jax.random.uniform(jax.random.fold_in(jax.random.fold_in(key, 6), dim), (shards_of,), jnp.float32, smallest / len(shards), high / len(shards))
        return jnp.repeat(jnp.exp(steps), dims[dim] // shards_of).reshape((-1,) + (1,) * (len(dims) - dim - 1))

    gain = one(*shards[0])
    for cut in shards[1:]:
        gain = gain * one(*cut)
    return gain


def bell_draw(own_key, extent, scale, bound, pieces=(), dtype=jnp.bfloat16):
    result = jax.random.normal(own_key, extent, jnp.float32) * scale
    if len(pieces) > 0:
        result = steps_of(own_key, extent, pieces, -0.22, 0.18) * result
    return jnp.clip(result, min=-bound, max=bound).astype(dtype)


def setup_inputs(seed: int = 0) -> dict:
    splits = jax.random.split(jax.random.key(seed), 6)
    gradients = bell_draw(splits[0], (TOKENS, OUT_DIM), 1.0, 6.0, ((0, 16), (1, 32)))
    activations = bell_draw(splits[1], (TOKENS, IN_DIM), 1.0, 6.0, ((0, 32), (1, 16)))
    out_basis = bell_draw(splits[2], (OUT_DIM, EIG_OUT), OUT_DIM ** -0.5, 0.03125, ((0, 32), (1, 16)))
    in_basis = bell_draw(splits[3], (IN_DIM, IN_DIM), IN_DIM ** -0.5, 0.0625, ((0, 16), (1, 32)))
    eigen_table = jnp.clip(jnp.exp(math.log(2.0) - 2.9957323 * jax.random.uniform(splits[4], (EIG_OUT, IN_DIM), jnp.float32) ** steps_of(splits[4], (EIG_OUT, IN_DIM), ((0, 16), (1, 32)), -0.2, 0.2)), 0.1, 2.0)
    return {"gradients": gradients, "activations": activations, "out_basis": out_basis, "in_basis": in_basis, "eigen_table": eigen_table}


def reference(gradients, activations, out_basis, in_basis, eigen_table):
    rotated_grad = jnp.dot(gradients, out_basis, preferred_element_type=jnp.float32).astype(jnp.bfloat16)
    rotated_act = jnp.dot(activations, in_basis, preferred_element_type=jnp.float32).astype(jnp.bfloat16)
    grad_blocks = rotated_grad.reshape(SEQS, LEN, EIG_OUT)
    act_blocks = rotated_act.reshape(SEQS, LEN, IN_DIM)

    def accumulate(total, pair):
        grad_seq, act_seq = pair
        corr = jnp.dot(grad_seq.T, act_seq, preferred_element_type=jnp.float32)
        return total + corr * corr, None

    total, unused = lax.scan(accumulate, jnp.zeros((EIG_OUT, IN_DIM), jnp.float32), (grad_blocks, act_blocks))
    return eigen_table + total / (SEQS * LEN)
```

```python
import jax
import jax.numpy as jnp
from jax import lax
from jax.sharding import Mesh, PartitionSpec as P

LEN = 128
OUT = ("xh", "y")
CHIPS = ("xl", "z")


def swap(value):
    return lax.ppermute(value, "c", [(0, 1), (1, 0)])


def exchange(pieces, axes):
    return lax.all_to_all(pieces, axes, 0, 0, tiled=True)


def spread(value, axes):
    size = lax.axis_size(axes)
    return exchange(jnp.broadcast_to(value[None], (size, *value.shape)), axes)


def reduce_rows(partial, axes):
    size = lax.axis_size(axes)
    rows, columns = partial.shape
    pieces = partial.astype(jnp.bfloat16).reshape(size, rows // size, columns)
    received = exchange(pieces, axes)
    return jnp.sum(received.astype(jnp.float32), axis=0).astype(jnp.bfloat16)


def local(gradients, activations, out_basis, in_basis, eigen_table):
    f32 = jnp.float32
    core = lax.axis_index("c")
    rows, features = gradients.shape
    half = rows // 2
    mine = lax.dynamic_slice_in_dim(gradients, core * half, half, 0)
    theirs = lax.dynamic_slice_in_dim(gradients, (1 - core) * half, half, 0)
    wide = jnp.concatenate([mine, swap(theirs)], axis=1)
    basis_other = swap(out_basis)

    wide = spread(wide, OUT)
    wide = wide.reshape(-1, wide.shape[2])
    partial_grad = jnp.dot(wide[:, :features], out_basis, preferred_element_type=f32)
    partial_grad += jnp.dot(wide[:, features:], basis_other, preferred_element_type=f32)
    grad_rows = reduce_rows(partial_grad, CHIPS)
    grads = spread(grad_rows, CHIPS)
    grads = jnp.stack([grads, swap(grads)], axis=1)

    acts = spread(activations, CHIPS)
    acts = acts.reshape(-1, acts.shape[2])
    acts = jnp.concatenate([acts, swap(acts)], axis=0)
    partial_act = jnp.dot(acts, in_basis, preferred_element_type=f32)
    act_rows = reduce_rows(partial_act, OUT)
    acts = spread(act_rows, OUT).reshape(2, -1, half, act_rows.shape[1])
    acts = jnp.stack([acts[0], acts[1]], axis=1)

    token_count = rows * lax.axis_size(OUT)
    grad_blocks = grads.reshape(token_count // LEN, LEN, grads.shape[-1])
    act_blocks = acts.reshape(token_count // LEN, LEN, acts.shape[-1])
    corr = jnp.einsum("stn,stm->snm", grad_blocks, act_blocks, preferred_element_type=f32)
    return eigen_table + jnp.sum(corr * corr, axis=0) / token_count


def solution(mesh):
    chips = Mesh(mesh.devices.reshape(2, 8, 2, 8, 2), ("xh", "y", "xl", "z", "c"))
    out_axes, in_axes = ("xh", "y"), ("xl", "z", "c")
    by_out, by_in = P(out_axes, in_axes), P(in_axes, out_axes)
    return jax.shard_map(
        local,
        mesh=chips,
        in_specs=(by_out, by_in, by_in, by_out, by_out),
        out_specs=by_out,
        check_vma=False,
    )
```
